32 devices in a mesh: io: 8 (over z, y), cmp: 4 (over x, core).
Axes of the slice: x: 2, y: 2, z: 4, core: 2. Of those that a mesh axis runs over, the one named last changes fastest.
Arguments:
- fields: float32 [6, 8, 512, 4096], P(None, None, 'cmp', 'io'), may hold values from -6 to 6
- mean_old: float32 [6, 8, 512, 3072], P(None, 'cmp', 'io'), may hold values from -6 to 6
- land_mask: int32 [8, 512, 4096], P('cmp', 'io'), may hold values from 0 to 1, as said below
Outputs:
- mean_new: float32 [6, 8, 512, 3072], P(None, 'cmp', 'io')
- level_rms: float32 [6, 8], P(None, 'cmp')
The draws below stay inside these ranges and needn't reach their ends.
Inputs may be any that keep to these rules, and one draw needn't show every extreme that they name: `land_mask`: each row (level, latitude) has between 1 and 3072 ocean points, and some row has exactly 3072.
All inputs are finite; a program needn't handle non-finite values.
Results may differ from the reference program's by a relative error of at most 0.00002.
Values sent between devices are 32-bit elements; how exact they have to be, the bound alone decides.
A program may use at most 128 MiB of HBM per device.

```python
import jax
import jax.numpy as jnp
from jax import lax

FIELDS = 6
NI = 4096
L = 8
STEPS = 3
NJ = 512
W = 3072


def draw_land_mask(key, part):
    key_scale, key_lev, key_row, key_perm = jax.random.split(jax.random.fold_in(key, 17), 4)
    row_index = jnp.arange(NJ, dtype=jnp.int32)
    base = W * (NJ + 3 * row_index) // (4 * NJ)
    factor = jax.random.randint(key_scale, (L, NJ), 80, 101)
    counts = jnp.maximum(base[None, :] * factor // 100, 1)
    pick_level = jax.random.randint(key_lev, (), 0, L)
    pick_row = jax.random.randint(key_row, (), 0, NJ)
    chosen = (jnp.arange(L, dtype=jnp.int32)[:, None] == pick_level) & (row_index[None, :] == pick_row)
    counts = jnp.where(chosen, W, counts)
    order = jnp.broadcast_to(jnp.arange(NI, dtype=jnp.int32), (L, NJ, NI))
    shuffled = jax.random.permutation(key_perm, order, axis=-1, independent=True)
    return (shuffled < counts[:, :, None]).astype(jnp.int32)


def shard_levels(own_key, shape, cuts, least, top_value):
    level = 1.0
    for dim, blocks in cuts:
        steps = jax.random.uniform(jax.random.fold_in(jax.random.fold_in(own_key, 6), dim), (blocks,), jnp.float32, least / len(cuts), top_value / len(cuts))
        level = level * jnp.repeat(jnp.exp(steps), shape[dim] // blocks).reshape((-1,) + (1,) * (len(shape) - 1 - dim))
    return level


def noise(stream_key, shape, spread, bound, cuts=(), kind=jnp.bfloat16):
    drawn = spread * jax.random.normal(stream_key, shape, jnp.float32)
    if cuts:
        drawn = drawn * shard_levels(stream_key, shape, cuts, -0.22, 0.18)
    return jnp.clip(drawn, -bound, bound).astype(kind)


def setup_inputs(seed: int = 0) -> dict:
    key_of = jax.random.split(jax.random.key(seed), 4)
    fields = noise(key_of[0], (FIELDS, L, NJ, NI), 1.0, 6.0, ((2, 4), (3, 8)), jnp.float32)
    mean_old = noise(key_of[1], (FIELDS, L, NJ, W), 1.0, 6.0, ((1, 4), (2, 8)), jnp.float32)
    land_mask = draw_land_mask(jax.random.fold_in(key_of[3], 71), 0)
    return dict(fields=fields, mean_old=mean_old, land_mask=land_mask)


def pack_one(values, target):
    width_out = 3 * values.shape[-1] // 4
    return jnp.zeros((values.shape[0], width_out), jnp.float32).at[:, target].set(values, mode='drop')

def pack_fields(fields, land_mask):
    nfield, nlev, nrow, ncol = fields.shape
    width_out = 3 * ncol // 4
    position = (jnp.cumsum(land_mask, axis=-1) - 1).astype(jnp.int32)
    target = jnp.where(land_mask == 1, position, width_out).astype(jnp.int32)
    flat = fields.reshape(nfield, nlev * nrow, ncol)
    packed = jax.vmap(pack_one, in_axes=(1, 0), out_axes=1)(flat, target.reshape(nlev * nrow, ncol))
    return packed.reshape(nfield, nlev, nrow, width_out)

def reference(fields, mean_old, land_mask):
    packed = pack_fields(fields, land_mask)
    counts = lax.optimization_barrier(jnp.sum(land_mask, axis=-1)).astype(jnp.int32)
    in_row = jnp.arange(mean_old.shape[-1], dtype=jnp.int32)[None, None, :] < counts[:, :, None]
    mean_new = jnp.where(in_row[None], (STEPS * mean_old + packed) / (STEPS + 1.0), jnp.float32(0.0))
    square_sum = lax.optimization_barrier(jnp.sum(mean_new * mean_new, axis=(2, 3)))
    ocean_total = lax.optimization_barrier(jnp.sum(counts, axis=1)).astype(jnp.float32)
    level_rms = jnp.sqrt(square_sum / ocean_total[None, :] + 1e-06)
    return (mean_new, level_rms)
```

```python
import functools

import jax
import jax.numpy as jnp
from jax import lax
from jax.experimental import pallas as pl
from jax.experimental.pallas import tpu as pltpu
from jax.sharding import PartitionSpec as P

STEPS = 3
LANES = 128
SUBS = 8
MESH = pl.DeviceIdType.MESH


def stages_of(count):
    return max(1, (count - 1).bit_length())


def lane_gather(array, index):
    return jnp.take_along_axis(array, index, axis=1, mode="promise_in_bounds")


def tile_rows(array):
    return jnp.concatenate(
        [array[:, t * LANES : (t + 1) * LANES] for t in range(array.shape[1] // LANES)], axis=0
    )


def tables(mask):
    rows = mask.shape[0]
    tiles = rows // SUBS
    lane = lax.broadcasted_iota(jnp.int32, (rows, LANES), 1)
    ranked = mask
    step = 1
    while step < LANES:
        ranked = ranked + jnp.where(lane >= step, pltpu.roll(ranked, step, 1), 0)
        step *= 2
    totals = jnp.broadcast_to(ranked[:, LANES - 1 :], (rows, LANES))
    bases = []
    base = jnp.zeros((SUBS, LANES), jnp.int32)
    for t in range(tiles):
        bases.append(base)
        base = base + totals[t * SUBS : (t + 1) * SUBS]
    counts = base
    base = jnp.concatenate(bases, axis=0)
    shift = jnp.where(mask == 1, lane - (ranked - 1), 0)
    step = 1
    while step < LANES:
        coming = pltpu.roll(shift, LANES - step, 1)
        shift = jnp.where(
            (coming & step) != 0, coming, jnp.where((shift & step) != 0, 0, shift)
        )
        step *= 2
    inside = (lane - base) & (LANES - 1)
    index = lane_gather((lane + shift) & (LANES - 1), inside)
    tile = lax.broadcasted_iota(jnp.int32, (rows, LANES), 0) // SUBS
    moves = jnp.where(inside < totals, tile - ((base + inside) >> 7), 0)
    bits = jnp.zeros((rows, LANES), jnp.int32)
    for k in range(stages_of(tiles)):
        amount = (1 << k) * SUBS
        if amount >= rows:
            break
        coming = jnp.concatenate(
            [moves[amount:], jnp.zeros((amount, LANES), jnp.int32)], axis=0
        )
        arrive = coming & (1 << k)
        bits = bits | arrive
        moves = jnp.where(
            arrive != 0, coming, jnp.where((moves & (1 << k)) != 0, 0, moves)
        )
    return index, bits, counts


def pack_rows(values, index, bits):
    rows = values.shape[0]
    tiles = rows // SUBS
    values = lane_gather(values, index)
    for k in range(stages_of(tiles)):
        amount = (1 << k) * SUBS
        if amount >= rows:
            break
        keep = rows - amount
        moved = jnp.where(
            (bits[:keep] & (1 << k)) != 0, values[amount:], values[:keep]
        )
        values = jnp.concatenate([moved, values[keep:]], axis=0)
    return values


def kernel(
    nio,
    ncmp,
    fields,
    mean_old,
    land_mask,
    mean_new,
    level_rms,
    recv,
    mean,
    mask,
    index,
    bits,
    counts,
    part,
    parts,
    send_sem,
    recv_sem,
    old_sem,
    new_sem,
    mask_sem,
    psend_sem,
    precv_sem,
):
    nfield, _, nlev, band, width = recv.shape
    width_out = mean.shape[-1]
    out_tiles = width_out // LANES
    groups = band // SUBS
    ratio = nio // ncmp
    ndest = ratio * ncmp
    my_io = lax.axis_index("io")
    my_cmp = lax.axis_index("cmp")

    def target(d):
        return ratio * my_cmp + lax.rem(d, ratio), lax.div(d, ratio)

    def piece(f, d):
        return fields.at[
            f,
            pl.ds(lax.div(d, ratio) * nlev, nlev),
            pl.ds(pl.multiple_of(lax.rem(d, ratio) * band, SUBS), band),
            :,
        ]

    def remote(f, d):
        to_io, to_cmp = target(d)
        return pltpu.make_async_remote_copy(
            src_ref=piece(f, d),
            dst_ref=recv.at[f, my_io],
            send_sem=send_sem.at[f, d],
            recv_sem=recv_sem.at[f, my_io],
            device_id=(to_io, to_cmp),
            device_id_type=MESH,
        )

    def local(f, d):
        return pltpu.make_async_copy(piece(f, d), recv.at[f, my_io], recv_sem.at[f, my_io])

    def is_me(d):
        to_io, to_cmp = target(d)
        return jnp.logical_and(to_io == my_io, to_cmp == my_cmp)

    def over_sends(action):
        def of_field(f, _):
            def of_dest(n, _):
                action(f, lax.rem(n + my_io, ndest))
                return 0

            return lax.fori_loop(0, ndest, of_dest, 0)

        lax.fori_loop(0, nfield, of_field, 0)

    def start(f, d):
        @pl.when(is_me(d))
        def _():
            local(f, d).start()

        @pl.when(jnp.logical_not(is_me(d)))
        def _():
            remote(f, d).start()

    def finish(f, d):
        @pl.when(jnp.logical_not(is_me(d)))
        def _():
            remote(f, d).wait_send()

    over_sends(start)

    mask_copy = pltpu.make_async_copy(land_mask, mask, mask_sem)
    mask_copy.start()

    def old_copy(f):
        return pltpu.make_async_copy(mean_old.at[f], mean.at[f], old_sem.at[f])

    def new_copy(f):
        return pltpu.make_async_copy(mean.at[f], mean_new.at[f], new_sem.at[f])

    def start_old(f, _):
        old_copy(f).start()
        return 0

    lax.fori_loop(0, nfield, start_old, 0)
    mask_copy.wait()
    part[...] = jnp.zeros(part.shape, jnp.float32)

    lane0 = lax.broadcasted_iota(jnp.int32, (SUBS, LANES), 1) == 0

    def rows_of(r):
        return pl.ds(pl.multiple_of(r * SUBS, SUBS), SUBS)

    for l in range(nlev):

        def make_tables(r, total, l=l):
            one_index, one_bits, one_counts = tables(tile_rows(mask[l, rows_of(r), :]))
            index[l, r] = one_index
            bits[l, r] = one_bits
            counts[l, r] = one_counts
            return total + one_counts

        total = lax.fori_loop(0, groups, make_tables, jnp.zeros((SUBS, LANES), jnp.int32))
        total = jnp.where(lane0, total, 0).astype(jnp.float32)
        row = nfield * nlev + l
        part[row : row + 1, :] = jnp.sum(total, axis=0, keepdims=True)

    def of_field(f, _):
        def arrived(s, _):
            pltpu.make_async_copy(recv.at[f, s], recv.at[f, s], recv_sem.at[f, s]).wait()
            return 0

        lax.fori_loop(0, nio, arrived, 0)
        old_copy(f).wait()
        slot = lax.broadcasted_iota(jnp.int32, (out_tiles * SUBS, LANES), 0)
        slot = (slot // SUBS) * LANES + lax.broadcasted_iota(
            jnp.int32, (out_tiles * SUBS, LANES), 1
        )

        for l in range(nlev):

            def of_rows(r, squares, l=l):
                at = rows_of(r)
                values = jnp.concatenate(
                    [tile_rows(recv[f, s, l, at, :]) for s in range(nio)], axis=0
                )
                packed = pack_rows(values, index[l, r], bits[l, r])[: out_tiles * SUBS]
                old = tile_rows(mean[f, l, at, :])
                in_row = slot < jnp.concatenate([counts[l, r]] * out_tiles, axis=0)
                new = jnp.where(
                    in_row, (STEPS * old + packed) * (1.0 / (STEPS + 1.0)), jnp.float32(0.0)
                )
                for t in range(out_tiles):
                    one = new[t * SUBS : (t + 1) * SUBS]
                    mean[f, l, at, t * LANES : (t + 1) * LANES] = one
                    squares = squares + one * one
                return squares

            squares = lax.fori_loop(0, groups, of_rows, jnp.zeros((SUBS, LANES), jnp.float32))
            part[pl.ds(f * nlev + l, 1), :] = jnp.sum(squares, axis=0, keepdims=True)
        new_copy(f).start()
        return 0

    lax.fori_loop(0, nfield, of_field, 0)
    parts[my_io] = part[...]
    over_sends(finish)

    def part_copy(p):
        return pltpu.make_async_remote_copy(
            src_ref=part,
            dst_ref=parts.at[my_io],
            send_sem=psend_sem.at[p],
            recv_sem=precv_sem.at[my_io],
            device_id=(lax.rem(my_io + p, nio), my_cmp),
            device_id_type=MESH,
        )

    def start_part(p, _):
        part_copy(p).start()
        return 0

    def finish_part(p, _):
        part_copy(p).wait_send()
        source = lax.rem(my_io + p, nio)
        pltpu.make_async_copy(parts.at[source], parts.at[source], precv_sem.at[source]).wait()
        return 0

    lax.fori_loop(1, nio, start_part, 0)
    lax.fori_loop(1, nio, finish_part, 0)

    summed = parts[0]
    for s in range(1, nio):
        summed = summed + parts[s]
    summed = jnp.sum(summed, axis=1, keepdims=True)
    for l in range(nlev):
        ocean_total = summed[nfield * nlev + l : nfield * nlev + l + 1]
        for f in range(nfield):
            one = summed[f * nlev + l : f * nlev + l + 1]
            level_rms[f : f + 1, l : l + 1] = jnp.sqrt(one / ocean_total + 1e-06)

    def finish_new(f, _):
        new_copy(f).wait()
        return 0

    lax.fori_loop(0, nfield, finish_new, 0)


def on_device(nio, ncmp, fields, mean_old, land_mask):
    nfield, nlev, band, width_out = mean_old.shape
    width = fields.shape[-1]
    ncol = land_mask.shape[-1]
    groups = band // SUBS
    rows = ncol // LANES * SUBS
    ndest = nio // ncmp * ncmp
    padded = -(-(nfield + 1) * nlev // SUBS) * SUBS
    dma = pltpu.SemaphoreType.DMA
    return pl.pallas_call(
        functools.partial(kernel, nio, ncmp),
        out_shape=(
            jax.ShapeDtypeStruct(mean_old.shape, jnp.float32),
            jax.ShapeDtypeStruct((nfield, nlev), jnp.float32),
        ),
        in_specs=[pl.BlockSpec(memory_space=pl.ANY)] * 3,
        out_specs=(
            pl.BlockSpec(memory_space=pl.ANY),
            pl.BlockSpec(memory_space=pltpu.VMEM),
        ),
        scratch_shapes=[
            pltpu.VMEM((nfield, nio, nlev, band, width), jnp.float32),
            pltpu.VMEM((nfield, nlev, band, width_out), jnp.float32),
            pltpu.VMEM((nlev, band, ncol), jnp.int32),
            pltpu.VMEM((nlev, groups, rows, LANES), jnp.int32),
            pltpu.VMEM((nlev, groups, rows, LANES), jnp.int32),
            pltpu.VMEM((nlev, groups, SUBS, LANES), jnp.int32),
            pltpu.VMEM((padded, LANES), jnp.float32),
            pltpu.VMEM((nio, padded, LANES), jnp.float32),
            dma((nfield, ndest)),
            dma((nfield, nio)),
            dma((nfield,)),
            dma((nfield,)),
            dma,
            dma((nio,)),
            dma((nio,)),
        ],
        compiler_params=pltpu.CompilerParams(has_side_effects=True),
    )(fields, mean_old, land_mask)


def solution(mesh):
    in_specs = (P(None, None, "cmp", "io"), P(None, "cmp", "io", None), P("cmp", "io", None))
    out_specs = (P(None, "cmp", "io", None), P(None, "cmp"))
    return jax.shard_map(
        functools.partial(on_device, mesh.shape["io"], mesh.shape["cmp"]),
        mesh=mesh,
        in_specs=in_specs,
        out_specs=out_specs,
        check_vma=False,
    )
```
